32 devices in a mesh: trade: 4 (over z), node: 8 (over y, x, core).
Axes of the slice: x: 2, y: 2, z: 4, core: 2. Of those that a mesh axis runs over, the one named last changes fastest.
Arguments:
- values_in: float32 [1024, 16384], P('trade', 'node'), may hold values from 0 to 1
- prob_up: float32 [16, 16384], P(None, 'node'), may hold values from 0.1 to 0.3
- prob_down: float32 [16, 16384], P(None, 'node'), may hold values from 0.1 to 0.3
- discount: float32 [16, 16384], P(None, 'node'), may hold values from 0.9 to 1
- swap_rate: float32 [16, 16384], P(None, 'node'), may hold values from -3 to 3
- annuity: float32 [16, 16384], P(None, 'node'), may hold values from 0.5 to 2
- state_price: float32 [16384], P('node'), may hold values from 3.0517578e-05 to 0.00012207031
- exercise_step: int32 [1024, 4], P('trade'), may hold values from 0 to 15
- strike_bucket: int32 [1024], P('trade'), may hold values from 0 to 63
- notional_sign: int32 [1024], P('trade'), may hold values from 0 to 1
- strike_table: float32 [64], replicated, may hold values from -0.5 to 0.5
Outputs:
- values_out: float32 [1024, 16384], P(('trade', 'node'))
- prices: float32 [1024], P(('trade', 'node'))
- portfolio: float32 [], replicated
The draws below stay inside these ranges and needn't reach their ends.
All inputs are finite; a program needn't handle non-finite values.
Results may differ from the reference program's by a relative error of at most 0.0003.
Values sent between devices are 32-bit elements; how exact they have to be, the bound alone decides.
A program may use at most 128 MiB of HBM per device.

```python
import math
import jax
import jax.numpy as jnp
from jax import lax

TRADE_DEV = 256
STEPS = 16
EXDATES = 4
BUCKETS = 64
NODES = 16384
TRADES = 1024
N_TRADE = 4


def touch_ends(drawn, stream_key, low, top_value):
    shape = drawn.shape
    index_at = [jax.random.randint(jax.random.fold_in(stream_key, axis), (), 0, shape[axis]) for axis in range(len(shape))]
    drawn = drawn.at[tuple(index_at)].set(low)
    longest = shape.index(max(shape))
    index_at[longest] = (index_at[longest] + 1) % shape[longest]
    return drawn.at[tuple(index_at)].set(top_value)


def block_levels(rng, shape, cuts, least, largest):
    level, own = 1.0, jax.random.fold_in(rng, 6)
    for axis_at, shards_of in cuts:
        heights = jnp.exp(jax.random.uniform(jax.random.fold_in(own, axis_at), (shards_of,), jnp.float32, least / len(cuts), largest / len(cuts)))
        level = level * jnp.repeat(heights, shape[axis_at] // shards_of).reshape([-1 if axis == axis_at else 1 for axis in range(len(shape))])
    return level


def normal_values(own_key, dims, deviation, most, cuts=(), held_as=jnp.bfloat16):
    entries = jax.random.normal(own_key, dims, jnp.float32) * deviation
    if len(cuts) > 0:
        entries = block_levels(own_key, dims, cuts, -0.22, 0.18) * entries
    return jnp.clip(entries, min=-most, max=most).astype(held_as)


def setup_inputs(seed: int = 0) -> dict:
    arg_keys = jax.random.split(jax.random.key(seed), 12)
    values_in = jnp.clip(1.0 * jax.random.uniform(arg_keys[0], (TRADES, NODES), jnp.float32) ** block_levels(arg_keys[0], (TRADES, NODES), ((0, 4), (1, 8)), -0.2, 0.2), 0.0, 1.0)
    prob_up = jnp.clip(0.1 + 0.20000001043081284 * jax.random.uniform(arg_keys[1], (STEPS, NODES), jnp.float32) ** block_levels(arg_keys[1], (STEPS, NODES), ((1, 8),), -0.2, 0.2), 0.1, 0.3)
    prob_down = jnp.clip(0.1 + 0.20000001043081284 * jax.random.uniform(arg_keys[2], (STEPS, NODES), jnp.float32) ** block_levels(arg_keys[2], (STEPS, NODES), ((1, 8),), -0.2, 0.2), 0.1, 0.3)
    discount = jnp.clip(0.9 + 0.100000024 * jax.random.uniform(arg_keys[3], (STEPS, NODES), jnp.float32) ** block_levels(arg_keys[3], (STEPS, NODES), ((1, 8),), -0.2, 0.2), 0.9, 1.0)
    swap_rate = normal_values(arg_keys[4], (STEPS, NODES), 0.5, 3.0, ((1, 8),), jnp.float32)
    annuity = jnp.clip(jnp.exp(math.log(2.0) - 1.3862944 * jax.random.uniform(arg_keys[5], (STEPS, NODES), jnp.float32) ** block_levels(arg_keys[5], (STEPS, NODES), ((1, 8),), -0.2, 0.2)), 0.5, 2.0)
    state_price = jnp.clip(jnp.exp(math.log(0.00012207031) - 1.3862944 * jax.random.uniform(arg_keys[6], (NODES,), jnp.float32) ** block_levels(arg_keys[6], (NODES,), ((0, 8),), -0.2, 0.2)), 3.0517578125e-05, 0.00012207031)
    exercise_step = touch_ends(jax.random.randint(arg_keys[7], (TRADES, EXDATES), 0, STEPS), jax.random.fold_in(arg_keys[7], 1), 0, STEPS - 1).astype(jnp.int32)
    strike_bucket = touch_ends(jax.random.randint(arg_keys[8], (TRADES,), 0, BUCKETS), jax.random.fold_in(arg_keys[8], 1), 0, BUCKETS - 1).astype(jnp.int32)
    notional_sign = touch_ends(jax.random.randint(arg_keys[9], (TRADES,), 0, 2), jax.random.fold_in(arg_keys[9], 1), 0, 1).astype(jnp.int32)
    strike_table = jnp.clip(jax.random.uniform(arg_keys[10], (BUCKETS,), jnp.float32, -0.5, 0.5), -0.5, 0.5)
    return {"values_in": values_in, "prob_up": prob_up, "prob_down": prob_down, "discount": discount, "swap_rate": swap_rate, "annuity": annuity, "state_price": state_price, "exercise_step": exercise_step, "strike_bucket": strike_bucket, "notional_sign": notional_sign, "strike_table": strike_table}


def strikes_of(bucket, strike_table):
    levels = lax.broadcasted_iota(jnp.int32, (1, strike_table.shape[0]), 1)
    return jnp.sum(jnp.where(bucket[:, None] == levels, strike_table[None, :], jnp.zeros((), strike_table.dtype)), axis=1)


def roll_once(padded, prob_up, prob_down, discount_row):
    middle = 1.0 - prob_up - prob_down
    return discount_row * (prob_up * padded[:, 2:] + middle * padded[:, 1:-1] + prob_down * padded[:, :-2])


def exercise(values, active, strike, signs, swap_row, annuity_row):
    payoff = signs[:, None] * annuity_row[None, :] * (swap_row[None, :] - strike[:, None])
    return jnp.where(active[:, None], jnp.maximum(values, payoff), values)


def reference(values_in, prob_up, prob_down, discount, swap_rate, annuity, state_price, exercise_step, strike_bucket, notional_sign, strike_table):
    strike = strikes_of(strike_bucket, strike_table)
    signs = (2 * notional_sign - 1).astype(jnp.float32)

    def one_block(pieces):
        values, dates, strikes, sign_rows = pieces
        for step in range(STEPS):
            padded = jnp.pad(values, ((0, 0), (1, 1)))
            values = roll_once(padded, prob_up[step], prob_down[step], discount[step])
            active = jnp.any(dates == step, axis=1)
            values = exercise(values, active, strikes, sign_rows, swap_rate[step], annuity[step])
        block_prices = jnp.sum(values * state_price[None, :], axis=1)
        return values, block_prices

    shaped = (values_in.reshape(N_TRADE, TRADE_DEV, NODES), exercise_step.reshape(N_TRADE, TRADE_DEV, EXDATES), strike.reshape(N_TRADE, TRADE_DEV), signs.reshape(N_TRADE, TRADE_DEV))
    values_all, prices_all = lax.map(one_block, shaped)
    prices = prices_all.reshape(TRADES)
    portfolio = jnp.sum(prices) / TRADE_DEV
    return values_all.reshape(TRADES, NODES), prices, portfolio
```

```python
import functools
import jax
import jax.numpy as jnp
from jax import lax
from jax.experimental import pallas as pl
from jax.experimental.pallas import tpu as pltpu
from jax.sharding import PartitionSpec as P

LANES = 128
HALF = 64
SUB = 8
MESH = pl.DeviceIdType.MESH
NEVER = 1e30


def strikes_of(bucket, strike_table):
    levels = lax.broadcasted_iota(jnp.int32, (1, strike_table.shape[0]), 1)
    return jnp.sum(
        jnp.where(
            bucket[:, None] == levels, strike_table[None, :], jnp.zeros((), strike_table.dtype)
        ),
        axis=1,
    )


def flip(me, d, n):
    out = 0
    bit = 1
    while bit < n:
        mine, other = (me // bit) % 2, (d // bit) % 2
        out = out + bit * (mine + other - 2 * mine * other)
        bit *= 2
    return out


def kernel(
    n, m, steps, rows, width,
    values_ref, up_ref, down_ref, disc_ref, swap_ref, ann_ref, price_ref, table_ref,
    out_ref, small_ref,
    vals, halo_v, raw, halo_c, coef, res, pacc, pmsg, precv, ztot, zrecv,
    in_sem, hs_sem, hr_sem, send_sem, recv_sem, self_sem, zs_sem, zr_sem, ps_sem, pr_sem,
):
    t = lax.axis_index("trade")
    me = lax.axis_index("node")
    block = rows if rows < 16 else 16
    parts = rows // block
    groups = block // SUB
    tiles = width // LANES
    lattice = (up_ref, down_ref, disc_ref, swap_ref, ann_ref)

    loads = [pltpu.make_async_copy(values_ref, vals, in_sem.at[0])]
    for k, ref in enumerate(lattice):
        loads.append(pltpu.make_async_copy(ref, raw.at[k], in_sem.at[1 + k]))
    for copy in loads:
        copy.start()

    barrier = pltpu.get_barrier_semaphore()
    for d in range(1, n):
        pl.semaphore_signal(barrier, inc=1, device_id=(t, (me + d) % n), device_id_type=MESH)
    for d in range(1, m):
        pl.semaphore_signal(barrier, inc=1, device_id=((t + d) % m, me), device_id_type=MESH)
    pl.semaphore_wait(barrier, n + m - 2)

    sides = ((0, (me + n - 1) % n, 0), (1, (me + 1) % n, width - LANES))
    halos = []
    for slot, target, first in sides:
        for k, ref in enumerate(lattice):
            halos.append(pltpu.make_async_remote_copy(
                src_ref=ref.at[:, pl.ds(first, LANES)], dst_ref=halo_c.at[slot, k],
                send_sem=hs_sem.at[slot, k], recv_sem=hr_sem.at[slot, k],
                device_id=(t, target), device_id_type=MESH))
    for slot, target, first in sides:
        halos.append(pltpu.make_async_remote_copy(
            src_ref=values_ref.at[:, pl.ds(first, LANES)], dst_ref=halo_v.at[slot],
            send_sem=hs_sem.at[slot, 5], recv_sem=hr_sem.at[slot, 5],
            device_id=(t, target), device_id_type=MESH))
    for copy in halos:
        copy.start()

    pmsg[...] = jnp.zeros_like(pmsg)

    def put_coefs(source, columns):
        up, down, disc, swap, ann = source
        rows_of = (disc * up, disc * (1.0 - up - down), disc * down, ann * swap, ann)
        for s in range(steps):
            for k in range(5):
                row = rows_of[k][s:s + 1, :]
                coef[s, k, :, columns] = jnp.broadcast_to(row, (SUB, row.shape[1]))

    for copy in loads[1:]:
        copy.wait()
    for i in range(tiles):
        cols = slice(i * LANES, (i + 1) * LANES)
        put_coefs([raw[k, :, cols] for k in range(5)], cols)
    loads[0].wait()

    lane = lax.broadcasted_iota(jnp.int32, (SUB, LANES), 1)
    has_right = jnp.where(me < n - 1, 1, 0)
    has_left = jnp.where(me > 0, 1, 0)

    def halo_mask(shape):
        at = lax.broadcasted_iota(jnp.int32, shape, 1)
        return jnp.where(at < HALF, has_right, has_left) > 0, at < HALF

    for copy in halos:
        copy.wait_recv()
    inside, right = halo_mask((steps, LANES))
    put_coefs(
        [jnp.where(inside, jnp.where(right, halo_c[0, k], halo_c[1, k]), 0.0) for k in range(5)],
        slice(width, width + LANES),
    )
    inside, right = halo_mask((SUB, LANES))
    first_lane = lane == 0
    last_lane = lane == LANES - 1

    def roll_block(row):
        start, tabs = [], []
        for g in range(groups):
            at = pl.ds(pl.multiple_of(row + g * SUB, SUB), SUB)
            line = [vals[at, i * LANES:(i + 1) * LANES] for i in range(tiles)]
            line.append(jnp.where(inside, jnp.where(right, halo_v[0, at, :], halo_v[1, at, :]), 0.0))
            start.append(line)
            tabs.append(table_ref[at, :])

        def step(s, carry):
            lines, tabs = carry
            new_lines, new_tabs = [], []
            for g in range(groups):
                sign = jnp.broadcast_to(tabs[g][:, 0:1], (SUB, LANES))
                level = jnp.broadcast_to(tabs[g][:, HALF:HALF + 1], (SUB, LANES))
                new_tabs.append(pltpu.roll(tabs[g], LANES - 1, 1))
                line = lines[g]
                ahead = [pltpu.roll(v, LANES - 1, 1) for v in line]
                behind = [pltpu.roll(v, 1, 1) for v in line]
                new = []
                for i in range(tiles + 1):
                    cols = slice(i * LANES, (i + 1) * LANES)
                    above = jnp.where(last_lane, ahead[(i + 1) % (tiles + 1)], ahead[i])
                    below = jnp.where(first_lane, behind[i - 1], behind[i])
                    rolled = (
                        coef[s, 0, :, cols] * above
                        + coef[s, 1, :, cols] * line[i]
                        + coef[s, 2, :, cols] * below
                    )
                    payoff = sign * coef[s, 3, :, cols] - level * coef[s, 4, :, cols]
                    new.append(jnp.maximum(rolled, payoff))
                new_lines.append(new)
            return new_lines, new_tabs

        lines, _ = lax.fori_loop(0, steps, step, (start, tabs))
        for g in range(groups):
            at = pl.ds(pl.multiple_of(row + g * SUB, SUB), SUB)
            total = jnp.zeros((SUB, LANES), jnp.float32)
            for i in range(tiles):
                cols = slice(i * LANES, (i + 1) * LANES)
                res[at, cols] = lines[g][i]
                total = total + lines[g][i] * price_ref[0:1, cols]
            pacc[at, :] = total

    def remote(d, h):
        dest = flip(me, d, n)
        return pltpu.make_async_remote_copy(
            src_ref=res.at[pl.ds(pl.multiple_of(dest * rows + h * block, SUB), block), :],
            dst_ref=out_ref.at[pl.ds(h * block, block), pl.ds(pl.multiple_of(me * width, LANES), width)],
            send_sem=send_sem.at[d, h], recv_sem=recv_sem.at[d, h],
            device_id=(t, dest), device_id_type=MESH)

    def at_home(h):
        return pltpu.make_async_copy(
            res.at[pl.ds(pl.multiple_of(me * rows + h * block, SUB), block), :],
            out_ref.at[pl.ds(h * block, block), pl.ds(pl.multiple_of(me * width, LANES), width)],
            self_sem.at[h])

    order = sum(d * 8 ** p for p, d in enumerate((2, 4, 3, 5, 6, 7, 1, 0)))

    def one_partner(p, code):
        d = code % 8 if n == 8 else (p + 2) % n
        dest = flip(me, d, n)
        for h in range(parts):
            roll_block(dest * rows + h * block)

            @pl.when(d > 0)
            def _():
                remote(d, h).start()

            @pl.when(d == 0)
            def _():
                at_home(h).start()
        return code // 8

    lax.fori_loop(0, n, one_partner, jnp.int32(order if n == 8 else 0))

    total = jnp.zeros((SUB, LANES), jnp.float32)
    for g in range(n * rows // SUB):
        total = total + pacc[g * SUB:(g + 1) * SUB, :]
    ztot[...] = total
    zcopies = []
    for d in range(1, m):
        zcopies.append(pltpu.make_async_remote_copy(
            src_ref=ztot, dst_ref=zrecv.at[d - 1],
            send_sem=zs_sem.at[d - 1], recv_sem=zr_sem.at[d - 1],
            device_id=((t + d) % m, me), device_id_type=MESH))
    for copy in zcopies:
        copy.start()
    ones = jnp.ones((SUB, LANES), jnp.float32)
    for d in range(n):
        dest = flip(me, d, n)
        mine = pacc[pl.ds(pl.multiple_of(dest * rows, SUB), rows), :]
        pmsg[d, 0:SUB, 0:rows] = lax.dot_general(
            ones, mine, (((1,), (1,)), ((), ())),
            precision=lax.Precision.HIGHEST, preferred_element_type=jnp.float32)
    for copy in zcopies:
        copy.wait_recv()
    for d in range(1, m):
        total = total + zrecv[d - 1]
    for d in range(n):
        pmsg[d, SUB:2 * SUB, :] = total
    pcopies = []
    for d in range(1, n):
        pcopies.append(pltpu.make_async_remote_copy(
            src_ref=pmsg.at[d], dst_ref=precv.at[d - 1],
            send_sem=ps_sem.at[d - 1], recv_sem=pr_sem.at[d - 1],
            device_id=(t, flip(me, d, n)), device_id_type=MESH))
    for copy in pcopies:
        copy.start()
    both = pmsg[0]
    for d, copy in enumerate(pcopies):
        copy.wait_recv()
        both = both + precv[d]
    small_ref[0:SUB, :] = both[0:SUB]
    small_ref[SUB:2 * SUB, :] = jnp.broadcast_to(
        jnp.sum(both[SUB:2 * SUB], keepdims=True) / (n * rows), (SUB, LANES))

    def drain(d, _):
        for h in range(parts):
            remote(d, h).wait()
        return 0

    lax.fori_loop(1, n, drain, 0)
    for h in range(parts):
        at_home(h).wait()
    for copy in halos + zcopies + pcopies:
        copy.wait_send()


def local(
    values_in, prob_up, prob_down, discount, swap_rate, annuity, state_price,
    exercise_step, strike_bucket, notional_sign, strike_table,
):
    n, m = lax.axis_size("node"), lax.axis_size("trade")
    steps = prob_up.shape[0]
    trades, width = values_in.shape
    rows = trades // n
    assert steps <= HALF and n & (n - 1) == 0
    block = min(rows, 16)

    strike = strikes_of(strike_bucket, strike_table)
    signs = (2 * notional_sign - 1).astype(jnp.float32)
    at = lax.broadcasted_iota(jnp.int32, (1, LANES), 1)
    active = jnp.any(exercise_step[:, :, None] == (at % HALF)[None], axis=1)
    table = jnp.where(
        at < HALF,
        jnp.where(active, signs[:, None], 0.0),
        jnp.where(active, (signs * strike)[:, None], NEVER),
    )

    hbm = pl.BlockSpec(memory_space=pl.ANY)
    vmem = pl.BlockSpec(memory_space=pltpu.VMEM)
    dma = pltpu.SemaphoreType.DMA
    f32 = jnp.float32
    out, small = pl.pallas_call(
        functools.partial(kernel, n, m, steps, rows, width),
        out_shape=(
            jax.ShapeDtypeStruct((rows, n * width), f32),
            jax.ShapeDtypeStruct((2 * SUB, LANES), f32),
        ),
        in_specs=[hbm] * 6 + [vmem] * 2,
        out_specs=(hbm, vmem),
        scratch_shapes=[
            pltpu.VMEM((trades, width), f32),
            pltpu.VMEM((2, trades, LANES), f32),
            pltpu.VMEM((5, steps, width), f32),
            pltpu.VMEM((2, 5, steps, LANES), f32),
            pltpu.VMEM((steps, 5, SUB, width + LANES), f32),
            pltpu.VMEM((trades, width), f32),
            pltpu.VMEM((trades, LANES), f32),
            pltpu.VMEM((n, 2 * SUB, LANES), f32),
            pltpu.VMEM((n - 1, 2 * SUB, LANES), f32),
            pltpu.VMEM((SUB, LANES), f32),
            pltpu.VMEM((m - 1, SUB, LANES), f32),
            dma((6,)), dma((2, 6)), dma((2, 6)),
            dma((n, rows // block)), dma((n, rows // block)), dma((rows // block,)),
            dma((m - 1,)), dma((m - 1,)), dma((n - 1,)), dma((n - 1,)),
        ],
        compiler_params=pltpu.CompilerParams(
            collective_id=0, has_side_effects=True, vmem_limit_bytes=40 * 1024 * 1024
        ),
        name="rollback",
    )(values_in, prob_up, prob_down, discount, swap_rate, annuity, state_price[None, :], table)
    return out, small[0, :rows], small[SUB, 0]


def solution(mesh):
    in_specs = (
        P("trade", "node"),
        P(None, "node"),
        P(None, "node"),
        P(None, "node"),
        P(None, "node"),
        P(None, "node"),
        P("node"),
        P("trade", None),
        P("trade"),
        P("trade"),
        P(),
    )
    out_specs = (P(("trade", "node"), None), P(("trade", "node")), P())
    return jax.shard_map(local, mesh=mesh, in_specs=in_specs, out_specs=out_specs, check_vma=False)
```

```python
import functools
import jax
import jax.numpy as jnp
from jax import lax
from jax.experimental import pallas as pl
from jax.experimental.pallas import tpu as pltpu
from jax.sharding import PartitionSpec as P

LANES = 128
HALF = 64
SUB = 8
MESH = pl.DeviceIdType.MESH
NEVER = 1e30


def strikes_of(bucket, strike_table):
    levels = lax.broadcasted_iota(jnp.int32, (1, strike_table.shape[0]), 1)
    return jnp.sum(
        jnp.where(
            bucket[:, None] == levels, strike_table[None, :], jnp.zeros((), strike_table.dtype)
        ),
        axis=1,
    )


def flip(me, d, n):
    out = 0
    bit = 1
    while bit < n:
        mine, other = (me // bit) % 2, (d // bit) % 2
        out = out + bit * (mine + other - 2 * mine * other)
        bit *= 2
    return out


def kernel(
    n, m, steps, rows, width,
    values_ref, up_ref, down_ref, disc_ref, swap_ref, ann_ref, price_ref, table_ref,
    out_ref, small_ref,
    vals, halo_v, raw, halo_c, coef, res, pacc, pmsg, precv, ztot, zrecv,
    in_sem, hs_sem, hr_sem, send_sem, recv_sem, self_sem, zs_sem, zr_sem, ps_sem, pr_sem,
):
    t = lax.axis_index("trade")
    me = lax.axis_index("node")
    block = rows if rows < 16 else 16
    parts = rows // block
    groups = block // SUB
    tiles = width // LANES
    lattice = (up_ref, down_ref, disc_ref, swap_ref, ann_ref)

    loads = [pltpu.make_async_copy(values_ref, vals, in_sem.at[0])]
    for k, ref in enumerate(lattice):
        loads.append(pltpu.make_async_copy(ref, raw.at[k], in_sem.at[1 + k]))
    for copy in loads:
        copy.start()

    barrier = pltpu.get_barrier_semaphore()
    for d in range(1, n):
        pl.semaphore_signal(barrier, inc=1, device_id=(t, (me + d) % n), device_id_type=MESH)
    for d in range(1, m):
        pl.semaphore_signal(barrier, inc=1, device_id=((t + d) % m, me), device_id_type=MESH)
    pl.semaphore_wait(barrier, n + m - 2)

    sides = ((0, (me + n - 1) % n, 0), (1, (me + 1) % n, width - LANES))
    halos = []
    for slot, target, first in sides:
        for k, ref in enumerate(lattice):
            halos.append(pltpu.make_async_remote_copy(
                src_ref=ref.at[:, pl.ds(first, LANES)], dst_ref=halo_c.at[slot, k],
                send_sem=hs_sem.at[slot, k], recv_sem=hr_sem.at[slot, k],
                device_id=(t, target), device_id_type=MESH))
    for slot, target, first in sides:
        halos.append(pltpu.make_async_remote_copy(
            src_ref=values_ref.at[:, pl.ds(first, LANES)], dst_ref=halo_v.at[slot],
            send_sem=hs_sem.at[slot, 5], recv_sem=hr_sem.at[slot, 5],
            device_id=(t, target), device_id_type=MESH))
    for copy in halos:
        copy.start()

    pmsg[...] = jnp.zeros_like(pmsg)

    def put_coefs(source, columns):
        up, down, disc, swap, ann = source
        rows_of = (disc * up, disc * (1.0 - up - down), disc * down, ann * swap, ann)
        for s in range(steps):
            for k in range(5):
                row = rows_of[k][s:s + 1, :]
                coef[s, k, :, columns] = jnp.broadcast_to(row, (SUB, row.shape[1]))

    for copy in loads[1:]:
        copy.wait()
    for i in range(tiles):
        cols = slice(i * LANES, (i + 1) * LANES)
        put_coefs([raw[k, :, cols] for k in range(5)], cols)
    loads[0].wait()

    lane = lax.broadcasted_iota(jnp.int32, (SUB, LANES), 1)
    has_right = jnp.where(me < n - 1, 1, 0)
    has_left = jnp.where(me > 0, 1, 0)

    def halo_mask(shape):
        at = lax.broadcasted_iota(jnp.int32, shape, 1)
        return jnp.where(at < HALF, has_right, has_left) > 0, at < HALF

    for copy in halos:
        copy.wait_recv()
    inside, right = halo_mask((steps, LANES))
    put_coefs(
        [jnp.where(inside, jnp.where(right, halo_c[0, k], halo_c[1, k]), 0.0) for k in range(5)],
        slice(width, width + LANES),
    )
    inside, right = halo_mask((SUB, LANES))
    first_lane = lane == 0
    last_lane = lane == LANES - 1

    def roll_block(row):
        start, tabs = [], []
        for g in range(groups):
            at = pl.ds(pl.multiple_of(row + g * SUB, SUB), SUB)
            line = [vals[at, i * LANES:(i + 1) * LANES] for i in range(tiles)]
            line.append(jnp.where(inside, jnp.where(right, halo_v[0, at, :], halo_v[1, at, :]), 0.0))
            start.append(line)
            tabs.append(table_ref[at, :])

        def step(s, carry):
            lines, tabs = carry
            new_lines, new_tabs = [], []
            for g in range(groups):
                sign = jnp.broadcast_to(tabs[g][:, 0:1], (SUB, LANES))
                level = jnp.broadcast_to(tabs[g][:, HALF:HALF + 1], (SUB, LANES))
                new_tabs.append(pltpu.roll(tabs[g], LANES - 1, 1))
                line = lines[g]
                ahead = [pltpu.roll(v, LANES - 1, 1) for v in line]
                behind = [pltpu.roll(v, 1, 1) for v in line]
                new = []
                for i in range(tiles + 1):
                    cols = slice(i * LANES, (i + 1) * LANES)
                    above = jnp.where(last_lane, ahead[(i + 1) % (tiles + 1)], ahead[i])
                    below = jnp.where(first_lane, behind[i - 1], behind[i])
                    rolled = (
                        coef[s, 0, :, cols] * above
                        + coef[s, 1, :, cols] * line[i]
                        + coef[s, 2, :, cols] * below
                    )
                    payoff = sign * coef[s, 3, :, cols] - level * coef[s, 4, :, cols]
                    new.append(jnp.maximum(rolled, payoff))
                new_lines.append(new)
            return new_lines, new_tabs

        lines, _ = lax.fori_loop(0, steps, step, (start, tabs), unroll=4)
        for g in range(groups):
            at = pl.ds(pl.multiple_of(row + g * SUB, SUB), SUB)
            total = jnp.zeros((SUB, LANES), jnp.float32)
            for i in range(tiles):
                cols = slice(i * LANES, (i + 1) * LANES)
                res[at, cols] = lines[g][i]
                total = total + lines[g][i] * price_ref[0:1, cols]
            pacc[at, :] = total

    def remote(d, h):
        dest = flip(me, d, n)
        return pltpu.make_async_remote_copy(
            src_ref=res.at[pl.ds(pl.multiple_of(dest * rows + h * block, SUB), block), :],
            dst_ref=out_ref.at[pl.ds(h * block, block), pl.ds(pl.multiple_of(me * width, LANES), width)],
            send_sem=send_sem.at[d, h], recv_sem=recv_sem.at[d, h],
            device_id=(t, dest), device_id_type=MESH)

    def at_home(h):
        return pltpu.make_async_copy(
            res.at[pl.ds(pl.multiple_of(me * rows + h * block, SUB), block), :],
            out_ref.at[pl.ds(h * block, block), pl.ds(pl.multiple_of(me * width, LANES), width)],
            self_sem.at[h])

    order = sum(d * 8 ** p for p, d in enumerate((2, 4, 3, 5, 6, 7, 1, 0)))

    def one_partner(p, code):
        d = code % 8 if n == 8 else (p + 2) % n
        dest = flip(me, d, n)
        for h in range(parts):
            roll_block(dest * rows + h * block)

            @pl.when(d > 0)
            def _():
                remote(d, h).start()

            @pl.when(d == 0)
            def _():
                at_home(h).start()
        return code // 8

    lax.fori_loop(0, n, one_partner, jnp.int32(order if n == 8 else 0))

    total = jnp.zeros((SUB, LANES), jnp.float32)
    for g in range(n * rows // SUB):
        total = total + pacc[g * SUB:(g + 1) * SUB, :]
    ztot[...] = total
    zcopies = []
    for d in range(1, m):
        zcopies.append(pltpu.make_async_remote_copy(
            src_ref=ztot, dst_ref=zrecv.at[d - 1],
            send_sem=zs_sem.at[d - 1], recv_sem=zr_sem.at[d - 1],
            device_id=((t + d) % m, me), device_id_type=MESH))
    for copy in zcopies:
        copy.start()
    ones = jnp.ones((SUB, LANES), jnp.float32)
    for d in range(n):
        dest = flip(me, d, n)
        mine = pacc[pl.ds(pl.multiple_of(dest * rows, SUB), rows), :]
        pmsg[d, 0:SUB, 0:rows] = lax.dot_general(
            ones, mine, (((1,), (1,)), ((), ())),
            precision=lax.Precision.HIGHEST, preferred_element_type=jnp.float32)
    for copy in zcopies:
        copy.wait_recv()
    for d in range(1, m):
        total = total + zrecv[d - 1]
    for d in range(n):
        pmsg[d, SUB:2 * SUB, :] = total
    pcopies = []
    for d in range(1, n):
        pcopies.append(pltpu.make_async_remote_copy(
            src_ref=pmsg.at[d], dst_ref=precv.at[d - 1],
            send_sem=ps_sem.at[d - 1], recv_sem=pr_sem.at[d - 1],
            device_id=(t, flip(me, d, n)), device_id_type=MESH))
    for copy in pcopies:
        copy.start()
    both = pmsg[0]
    for d, copy in enumerate(pcopies):
        copy.wait_recv()
        both = both + precv[d]
    small_ref[0:SUB, :] = both[0:SUB]
    small_ref[SUB:2 * SUB, :] = jnp.broadcast_to(
        jnp.sum(both[SUB:2 * SUB], keepdims=True) / (n * rows), (SUB, LANES))

    def drain(d, _):
        for h in range(parts):
            remote(d, h).wait()
        return 0

    lax.fori_loop(1, n, drain, 0)
    for h in range(parts):
        at_home(h).wait()
    for copy in halos + zcopies + pcopies:
        copy.wait_send()


def local(
    values_in, prob_up, prob_down, discount, swap_rate, annuity, state_price,
    exercise_step, strike_bucket, notional_sign, strike_table,
):
    n, m = lax.axis_size("node"), lax.axis_size("trade")
    steps = prob_up.shape[0]
    trades, width = values_in.shape
    rows = trades // n
    assert steps <= HALF and n & (n - 1) == 0
    block = min(rows, 16)

    strike = strikes_of(strike_bucket, strike_table)
    signs = (2 * notional_sign - 1).astype(jnp.float32)
    at = lax.broadcasted_iota(jnp.int32, (1, LANES), 1)
    active = jnp.any(exercise_step[:, :, None] == (at % HALF)[None], axis=1)
    table = jnp.where(
        at < HALF,
        jnp.where(active, signs[:, None], 0.0),
        jnp.where(active, (signs * strike)[:, None], NEVER),
    )

    hbm = pl.BlockSpec(memory_space=pltpu.HBM)
    either = pl.BlockSpec(memory_space=pl.ANY)
    vmem = pl.BlockSpec(memory_space=pltpu.VMEM)
    dma = pltpu.SemaphoreType.DMA
    f32 = jnp.float32
    out, small = pl.pallas_call(
        functools.partial(kernel, n, m, steps, rows, width),
        out_shape=(
            jax.ShapeDtypeStruct((rows, n * width), f32),
            jax.ShapeDtypeStruct((2 * SUB, LANES), f32),
        ),
        in_specs=[hbm] * 6 + [vmem] * 2,
        out_specs=(either, vmem),
        scratch_shapes=[
            pltpu.VMEM((trades, width), f32),
            pltpu.VMEM((2, trades, LANES), f32),
            pltpu.VMEM((5, steps, width), f32),
            pltpu.VMEM((2, 5, steps, LANES), f32),
            pltpu.VMEM((steps, 5, SUB, width + LANES), f32),
            pltpu.VMEM((trades, width), f32),
            pltpu.VMEM((trades, LANES), f32),
            pltpu.VMEM((n, 2 * SUB, LANES), f32),
            pltpu.VMEM((n - 1, 2 * SUB, LANES), f32),
            pltpu.VMEM((SUB, LANES), f32),
            pltpu.VMEM((m - 1, SUB, LANES), f32),
            dma((6,)), dma((2, 6)), dma((2, 6)),
            dma((n, rows // block)), dma((n, rows // block)), dma((rows // block,)),
            dma((m - 1,)), dma((m - 1,)), dma((n - 1,)), dma((n - 1,)),
        ],
        compiler_params=pltpu.CompilerParams(
            collective_id=0, has_side_effects=True, vmem_limit_bytes=40 * 1024 * 1024
        ),
        name="rollback",
    )(values_in, prob_up, prob_down, discount, swap_rate, annuity, state_price[None, :], table)
    return out, small[0, :rows], small[SUB, 0]


def solution(mesh):
    in_specs = (
        P("trade", "node"),
        P(None, "node"),
        P(None, "node"),
        P(None, "node"),
        P(None, "node"),
        P(None, "node"),
        P("node"),
        P("trade", None),
        P("trade"),
        P("trade"),
        P(),
    )
    out_specs = (P(("trade", "node"), None), P(("trade", "node")), P())
    return jax.shard_map(local, mesh=mesh, in_specs=in_specs, out_specs=out_specs, check_vma=False)
```
